8 devices in a mesh: dp: 1 (over z), x: 2 (over y), y: 4 (over x, core).
Axes of the slice: x: 2, y: 2, z: 1, core: 2. Of those that a mesh axis runs over, the one named last changes fastest.
Arguments:
- hidden: bfloat16 [1024, 2048], P('dp', 'x')
- w_qkv: bfloat16 [2048, 6144], P('x', 'y')
- b_qkv: bfloat16 [6144], P('y')
- w_out: bfloat16 [2048, 2048], P('y', 'x')
- b_out: bfloat16 [2048], P('x')
- attn_gain: bfloat16 [2048], P('x')
- attn_shift: bfloat16 [2048], P('x')
- w_up: bfloat16 [2048, 2, 8192], P('x', None, 'y')
- b_up: bfloat16 [2, 8192], P(None, 'y')
- w_down: bfloat16 [8192, 2048], P('y', 'x')
- b_down: bfloat16 [2048], P('x')
- mlp_gain: bfloat16 [2048], P('x')
- mlp_shift: bfloat16 [2048], P('x')
- k_cache: bfloat16 [1024, 64, 32, 64], P('dp', None, 'y')
- v_cache: bfloat16 [1024, 64, 32, 64], P('dp', None, 'y')
- positions: int32 [1024], P('dp')
- lengths: int32 [1024], P('dp')
Outputs:
- output 1: bfloat16 [1024, 2048], P('dp', 'x')
- output 2: bfloat16 [1024, 64, 32, 64], P('dp', None, 'y')
- output 3: bfloat16 [1024, 64, 32, 64], P('dp', None, 'y')
All inputs are finite; a program needn't handle non-finite values.
Results may differ from the reference program's by a relative error of at most 0.02.
Values are sent between devices in bfloat16 or wider.
A program may use at most 1.25 GiB of HBM per device.

```python
import math
import jax
import jax.numpy as jnp
from jax import lax

D = 2048
HEADS = 32
HEAD = 64
FF = 8192
BATCH_ROWS = 1024
CACHE_LEN = 64

DEEP_ALPHA = math.sqrt(140.0)
LN_EPS = 1e-5
ROPE_BASE = 10000.0


def setup_inputs(seed: int = 0, part: int = 0) -> dict:
    root_key = jax.random.key(seed)
    weight_keys = jax.random.split(root_key, 12)
    part_keys = jax.random.split(jax.random.fold_in(root_key, part), 5)

    def draw_normal(key, shape, scale):
        return jax.random.normal(key, shape, jnp.float32) * scale

    col_ramp = 0.4 + 1.2 * jnp.arange(D, dtype=jnp.float32) / D
    hidden = (draw_normal(part_keys[0], (BATCH_ROWS, D), 1.0) * col_ramp).astype(jnp.bfloat16)
    w_qkv = draw_normal(weight_keys[0], (D, 3 * D), D ** -0.5).astype(jnp.bfloat16)
    b_qkv = draw_normal(weight_keys[1], (3 * D,), 0.5).astype(jnp.bfloat16)
    w_out = draw_normal(weight_keys[2], (D, D), 2.0 * DEEP_ALPHA * D ** -0.5).astype(jnp.bfloat16)
    b_out = draw_normal(weight_keys[3], (D,), 0.3 * DEEP_ALPHA).astype(jnp.bfloat16)
    attn_gain = (col_ramp * (1.0 + draw_normal(weight_keys[4], (D,), 0.2))).astype(jnp.bfloat16)
    attn_shift = draw_normal(weight_keys[5], (D,), 0.3).astype(jnp.bfloat16)
    w_up = draw_normal(weight_keys[6], (D, 2, FF), D ** -0.5).astype(jnp.bfloat16)
    b_up = draw_normal(weight_keys[7], (2, FF), 0.5).astype(jnp.bfloat16)
    w_down = draw_normal(weight_keys[8], (FF, D), 1.2 * DEEP_ALPHA * FF ** -0.5).astype(jnp.bfloat16)
    b_down = draw_normal(weight_keys[9], (D,), 0.3 * DEEP_ALPHA).astype(jnp.bfloat16)
    mlp_gain = (1.0 + draw_normal(weight_keys[10], (D,), 0.3)).astype(jnp.bfloat16)
    mlp_shift = draw_normal(weight_keys[11], (D,), 0.3).astype(jnp.bfloat16)
    k_cache = draw_normal(part_keys[1], (BATCH_ROWS, CACHE_LEN, HEADS, HEAD), 2.0).astype(jnp.bfloat16)
    v_cache = draw_normal(part_keys[2], (BATCH_ROWS, CACHE_LEN, HEADS, HEAD), 1.0).astype(jnp.bfloat16)
    lengths = jax.random.randint(part_keys[3], (BATCH_ROWS,), 0, CACHE_LEN, jnp.int32)
    lengths = lengths.at[0].set(CACHE_LEN - 1).at[1].set(0)
    offsets = jax.random.randint(part_keys[4], (BATCH_ROWS,), 0, CACHE_LEN, jnp.int32)
    offsets = offsets.at[2].set(CACHE_LEN - 1).at[3].set(0)
    positions = lengths + offsets
    return {'hidden': hidden, 'w_qkv': w_qkv, 'b_qkv': b_qkv, 'w_out': w_out, 'b_out': b_out, 'attn_gain': attn_gain, 'attn_shift': attn_shift, 'w_up': w_up, 'b_up': b_up, 'w_down': w_down, 'b_down': b_down, 'mlp_gain': mlp_gain, 'mlp_shift': mlp_shift, 'k_cache': k_cache, 'v_cache': v_cache, 'positions': positions, 'lengths': lengths}


def apply_rotary(head_vec, positions):
    half_dim = HEAD // 2
    inv_freq = ROPE_BASE ** (-2.0 * jnp.arange(half_dim, dtype=jnp.float32) / HEAD)
    angles = positions.astype(jnp.float32)[:, None] * inv_freq[None, :]
    cos_table = jnp.cos(angles)[:, None, :]
    sin_table = jnp.sin(angles)[:, None, :]
    vec_wide = head_vec.astype(jnp.float32)
    lower_half = vec_wide[..., :half_dim]
    upper_half = vec_wide[..., half_dim:]
    return jnp.concatenate([lower_half * cos_table - upper_half * sin_table, upper_half * cos_table + lower_half * sin_table], axis=-1).astype(jnp.bfloat16)


def layer_norm(h_val, gain, shift):
    mean_row = jnp.mean(h_val, axis=-1, keepdims=True)
    var_row = jnp.mean(jnp.square(h_val - mean_row), axis=-1, keepdims=True)
    return (h_val - mean_row) * lax.rsqrt(var_row + LN_EPS) * gain.astype(jnp.float32) + shift.astype(jnp.float32)


def reference(hidden, w_qkv, b_qkv, w_out, b_out, attn_gain, attn_shift, w_up, b_up, w_down, b_down, mlp_gain, mlp_shift, k_cache, v_cache, positions, lengths):
    qkv_vals = (jnp.dot(hidden, w_qkv, preferred_element_type=jnp.float32) + b_qkv.astype(jnp.float32)).astype(jnp.bfloat16)
    qkv_vals = qkv_vals.reshape(BATCH_ROWS, HEADS, 3, HEAD)
    query_rot = apply_rotary(qkv_vals[:, :, 0], positions)
    key_rot = apply_rotary(qkv_vals[:, :, 1], positions)
    slot_hit = (jnp.arange(CACHE_LEN)[None, :] == lengths[:, None])[:, :, None, None]
    k_full = jnp.where(slot_hit, key_rot[:, None], k_cache)
    v_full = jnp.where(slot_hit, qkv_vals[:, None, :, 2], v_cache)

    def attend_row(row_args):
        query_row, key_row, value_row, length_row = row_args
        scores = jnp.einsum('hd,shd->hs', query_row.astype(jnp.float32), key_row.astype(jnp.float32)) * (HEAD ** -0.5)
        slot_ok = jnp.arange(CACHE_LEN)[None, :] <= length_row
        scores = jnp.where(slot_ok, scores, -1e30)
        attn_probs = jax.nn.softmax(scores, axis=-1).astype(jnp.bfloat16).astype(jnp.float32)
        return jnp.einsum('hs,shd->hd', attn_probs, value_row.astype(jnp.float32)).astype(jnp.bfloat16)

    attn_out = lax.map(attend_row, (query_rot, k_full, v_full, lengths)).reshape(BATCH_ROWS, D)
    proj_sum = jnp.dot(attn_out, w_out, preferred_element_type=jnp.float32) + b_out.astype(jnp.float32)
    h_attn = DEEP_ALPHA * hidden.astype(jnp.float32) + proj_sum
    normed = layer_norm(h_attn, attn_gain, attn_shift).astype(jnp.bfloat16)
    up_sum = jnp.dot(normed, w_up.reshape(D, 2 * FF), preferred_element_type=jnp.float32).reshape(BATCH_ROWS, 2, FF) + b_up.astype(jnp.float32)
    gated_act = (jax.nn.gelu(up_sum[:, 0], approximate=True) * up_sum[:, 1]).astype(jnp.bfloat16)
    down_sum = jnp.dot(gated_act, w_down, preferred_element_type=jnp.float32)
    h_mlp = DEEP_ALPHA * normed.astype(jnp.float32) + down_sum + b_down.astype(jnp.float32)
    result = layer_norm(h_mlp, mlp_gain, mlp_shift).astype(jnp.bfloat16)
    return (result, k_full, v_full)
```

```python
import functools
import math
import jax
import jax.numpy as jnp
from jax import lax
from jax.experimental import pallas as pl
from jax.experimental.pallas import tpu as pltpu
from jax.sharding import PartitionSpec as P

DEEP_ALPHA = math.sqrt(140.0)
LN_EPS = 1e-5
ROPE_BASE = 10000.0
HEAD_CHUNKS = 4
UP_CHUNKS = 4
UP_DEPTH_CUTS = 2
STREAMS = 2
SLOT_BLOCK = 8
RING = 16
AHEAD = 8
LANES = 128
TILE = 8
F32 = jnp.float32
BF16 = jnp.bfloat16


def ring_step(t, total, fetch, store, work):
    slot = lax.rem(t, RING)
    fetch(t, slot, False)
    work(slot)
    store(t, slot, True)
    nxt = t + AHEAD
    nxt_slot = lax.rem(nxt, RING)

    @pl.when(jnp.logical_and(nxt < total, nxt >= RING))
    def _():
        store(nxt - RING, nxt_slot, False)

    @pl.when(nxt < total)
    def _():
        fetch(nxt, nxt_slot, True)


def insert_slots(buf, slot, first_slot, len_ref, new_ref, new_row, lane_start, use):
    head_dim = buf.shape[3]
    new_row = new_row if isinstance(new_row, int) else pl.multiple_of(new_row, head_dim)

    def lanes(lb, carry):
        cols = pl.ds(pl.multiple_of(lb * LANES, LANES), LANES)
        ahead = jnp.broadcast_to((len_ref[:, cols] - first_slot).astype(F32), (TILE, LANES)).astype(BF16)
        new = [new_ref[pl.ds(new_row + t, TILE), cols] for t in range(0, head_dim, TILE)]
        state = lane_start(cols)
        for i in range(SLOT_BLOCK):
            here = ahead == jnp.asarray(i, BF16)
            tiles = []
            for j, t in enumerate(range(0, head_dim, TILE)):
                tile = jnp.where(here, new[j], buf[slot, i, 0, t:t + TILE, cols])
                buf[slot, i, 0, t:t + TILE, cols] = tile
                tiles.append(tile)
            state = use(i, cols, tiles, state)
        return carry

    lax.fori_loop(0, len_ref.shape[1] // LANES, lanes, 0)


def attend_kernel(first_ref, own_ref, recv_ref, cos_ref, sin_ref, len_ref, k_ref, v_ref, *rest):
    k_out, v_out, attn_out, k_new_out, v_new_out, buf, query_s, part_s, prob_s, acc_s, in_sem, out_sem = rest[-12:]
    slots, head_dim, rows = k_ref.shape[0], k_ref.shape[2], k_ref.shape[3]
    half_dim = head_dim // 2
    heads = attn_out.shape[0] // head_dim
    groups = slots // SLOT_BLOCK
    total = heads * 2 * groups
    first_head = first_ref[0]

    def copies(t, slot, inward):
        h = first_head + t // (2 * groups)
        g = lax.rem(t, groups)
        at = (pl.ds(g * SLOT_BLOCK, SLOT_BLOCK), pl.ds(h, 1))
        pair = []
        for src, dst in ((k_ref, k_out), (v_ref, v_out)):
            if inward:
                pair.append(functools.partial(pltpu.make_async_copy, src.at[at], buf.at[slot], in_sem.at[slot]))
            else:
                pair.append(functools.partial(pltpu.make_async_copy, buf.at[slot], dst.at[at], out_sem.at[slot]))
        return pair

    def move(inward):
        def go(t, slot, start):
            k_copy, v_copy = copies(t, slot, inward)
            if not start:
                k_copy().wait()
                return
            is_k = lax.rem(t // groups, 2) == 0
            pl.when(is_k)(lambda: k_copy().start())
            pl.when(jnp.logical_not(is_k))(lambda: v_copy().start())

        return go

    fetch, store = move(True), move(False)
    for t in range(AHEAD):
        fetch(jnp.int32(t), jnp.int32(t), True)

    cos_t, sin_t = cos_ref[...], sin_ref[...]

    def rotate(vec):
        lower, upper = vec[:half_dim], vec[half_dim:]
        return jnp.concatenate([lower * cos_t - upper * sin_t, upper * cos_t + lower * sin_t], axis=0).astype(BF16)

    for h in range(heads):
        base = h * 3 * head_dim

        def piece(i):
            at = slice(base + i * head_dim, base + (i + 1) * head_dim)
            return (own_ref[at, :] + recv_ref[at, :].astype(F32)).astype(BF16)

        query_s[...] = rotate(piece(0).astype(F32)).astype(F32) * (head_dim ** -0.5)
        here = slice(h * head_dim, (h + 1) * head_dim)
        k_new_out[here, :] = rotate(piece(1).astype(F32))
        v_new_out[here, :] = piece(2)

        def k_group(g, carry):
            t = h * 2 * groups + g

            def use(i, cols, tiles, query):
                total_p = tiles[0].astype(F32) * query[0]
                for tile, q in zip(tiles[1:], query[1:]):
                    total_p = total_p + tile.astype(F32) * q
                part_s[g * SLOT_BLOCK + i, :, cols] = total_p
                return query

            def load_query(cols):
                return [query_s[d:d + TILE, cols] for d in range(0, head_dim, TILE)]

            ring_step(t, total, fetch, store, lambda slot: insert_slots(buf, slot, g * SLOT_BLOCK, len_ref, k_new_out, h * head_dim, load_query, use))
            return carry

        lax.fori_loop(0, groups, k_group, 0)

        def soft(lb, carry):
            cols = pl.ds(pl.multiple_of(lb * LANES, LANES), LANES)
            slot_ids = lax.broadcasted_iota(jnp.int32, (slots, LANES), 0)
            scores = jnp.sum(part_s[:, :, cols], axis=1)
            scores = jnp.where(slot_ids <= len_ref[:, cols], scores, -1e30)
            expd = jnp.exp(scores - jnp.max(scores, axis=0, keepdims=True))
            prob_s[:, cols] = (expd / jnp.sum(expd, axis=0, keepdims=True)).astype(BF16).astype(F32)
            acc_s[:, cols] = jnp.zeros((head_dim, LANES), F32)
            return carry

        lax.fori_loop(0, rows // LANES, soft, 0)

        def v_group(g, carry):
            t = h * 2 * groups + groups + g

            def load_acc(cols):
                probs = prob_s[pl.ds(pl.multiple_of(g * SLOT_BLOCK, SLOT_BLOCK), SLOT_BLOCK), cols]
                return probs, [acc_s[d:d + TILE, cols] for d in range(0, head_dim, TILE)]

            def use(i, cols, tiles, state):
                probs, acc = state
                prob = jnp.broadcast_to(probs[i:i + 1, :], (TILE, LANES))
                acc = [a + tile.astype(F32) * prob for a, tile in zip(acc, tiles)]
                if i == SLOT_BLOCK - 1:
                    for a, d in zip(acc, range(0, head_dim, TILE)):
                        acc_s[d:d + TILE, cols] = a
                return probs, acc

            ring_step(t, total, fetch, store, lambda slot: insert_slots(buf, slot, g * SLOT_BLOCK, len_ref, v_new_out, h * head_dim, load_acc, use))
            return carry

        lax.fori_loop(0, groups, v_group, 0)
        attn_out[here, :] = acc_s[...].astype(BF16)

    for t in range(max(total - RING, 0), total):
        store(jnp.int32(t), jnp.int32(t % RING), False)


def attend_chunk(first, heads, own, recv, cos_t, sin_t, len_row, k_cache, v_cache, k_prev, v_prev):
    slots, _, head_dim, rows = k_cache.shape
    args = [first, own, recv, cos_t, sin_t, len_row, k_cache, v_cache]
    vmem, hbm = pl.BlockSpec(memory_space=pltpu.VMEM), pl.BlockSpec(memory_space=pl.ANY)
    in_specs = [pl.BlockSpec(memory_space=pltpu.SMEM)] + [vmem] * 5 + [hbm] * 2
    aliases = {}
    if k_prev is not None:
        args += [k_prev, v_prev]
        in_specs += [hbm] * 2
        aliases = {8: 0, 9: 1}
    vec = jax.ShapeDtypeStruct((heads * head_dim, rows), BF16)
    return pl.pallas_call(
        attend_kernel,
        in_specs=in_specs,
        out_specs=[hbm, hbm, vmem, vmem, vmem],
        scratch_shapes=[pltpu.VMEM((RING, SLOT_BLOCK, 1, head_dim, rows), BF16), pltpu.VMEM((head_dim, rows), F32), pltpu.VMEM((slots, 8, rows), F32), pltpu.VMEM((slots, rows), F32), pltpu.VMEM((head_dim, rows), F32), pltpu.SemaphoreType.DMA((RING,)), pltpu.SemaphoreType.DMA((RING,))],
        out_shape=[jax.ShapeDtypeStruct(k_cache.shape, BF16), jax.ShapeDtypeStruct(v_cache.shape, BF16), vec, vec, vec],
        input_output_aliases=aliases,
        compiler_params=pltpu.CompilerParams(vmem_limit_bytes=40 * 2 ** 20),
        cost_estimate=pl.CostEstimate(flops=12_000_000_000 * heads, bytes_accessed=8 * heads * slots * head_dim * rows, transcendentals=0),
    )(*args)


def insert_kernel(first_ref, len_ref, new_ref, c_ref, prev_ref, c_out, buf, in_sem, out_sem):
    slots, head_dim = c_ref.shape[0], c_ref.shape[2]
    heads = new_ref.shape[0] // head_dim
    groups = slots // SLOT_BLOCK
    total = heads * groups
    first_head = first_ref[0]

    def move(inward):
        def go(t, slot, start):
            at = (pl.ds(lax.rem(t, groups) * SLOT_BLOCK, SLOT_BLOCK), pl.ds(first_head + t // groups, 1))
            if inward:
                copy = pltpu.make_async_copy(c_ref.at[at], buf.at[slot], in_sem.at[slot])
            else:
                copy = pltpu.make_async_copy(buf.at[slot], c_out.at[at], out_sem.at[slot])
            copy.start() if start else copy.wait()

        return go

    fetch, store = move(True), move(False)
    for t in range(AHEAD):
        fetch(jnp.int32(t), jnp.int32(t), True)

    def step(t, carry):
        h, g = t // groups, lax.rem(t, groups)
        row = pl.multiple_of(h * head_dim, head_dim)
        ring_step(t, total, fetch, store, lambda slot: insert_slots(buf, slot, g * SLOT_BLOCK, len_ref, new_ref, row, lambda cols: None, lambda i, cols, tiles, state: None))
        return carry

    lax.fori_loop(0, total, step, 0)
    for t in range(max(total - RING, 0), total):
        store(jnp.int32(t), jnp.int32(t % RING), False)


def insert_other(first, len_row, new, cache, prev):
    slots, _, head_dim, rows = cache.shape
    vmem, hbm = pl.BlockSpec(memory_space=pltpu.VMEM), pl.BlockSpec(memory_space=pl.ANY)
    return pl.pallas_call(
        insert_kernel,
        in_specs=[pl.BlockSpec(memory_space=pltpu.SMEM), vmem, vmem, hbm, hbm],
        out_specs=hbm,
        scratch_shapes=[pltpu.VMEM((RING, SLOT_BLOCK, 1, head_dim, rows), BF16), pltpu.SemaphoreType.DMA((RING,)), pltpu.SemaphoreType.DMA((RING,))],
        out_shape=jax.ShapeDtypeStruct(cache.shape, BF16),
        input_output_aliases={4: 0},
        compiler_params=pltpu.CompilerParams(vmem_limit_bytes=24 * 2 ** 20),
        cost_estimate=pl.CostEstimate(flops=5_000_000_000 * (new.shape[0] // head_dim), bytes_accessed=4 * slots * new.shape[0] * rows, transcendentals=0),
    )(first, len_row, new, cache, prev)


def relayout_kernel(block_ref, w_ref, *outs):
    step = pl.program_id(0)
    both = jnp.swapaxes(w_ref[...], 0, 1)
    width = outs[0].shape[2]
    per_cut = pl.num_programs(0) // UP_DEPTH_CUTS
    for i, out in enumerate(outs):
        f, cut = (i // UP_DEPTH_CUTS, i % UP_DEPTH_CUTS) if len(outs) > 1 else (0, None)

        def write(out=out, f=f):
            out[...] = both[:, :, f * width:(f + 1) * width]

        if cut is None:
            write()
        else:
            pl.when(step // per_cut == cut)(write)


def relayout_up(block, w_up, split):
    depth = w_up.shape[0]
    width = w_up.shape[2] // 2
    db = 128
    steps = depth // db
    per_cut = steps // UP_DEPTH_CUTS
    if split:
        fc = width // UP_CHUNKS
        outs = [jax.ShapeDtypeStruct((2, depth // UP_DEPTH_CUTS, fc), BF16)] * (UP_CHUNKS * UP_DEPTH_CUTS)
        specs = [pl.BlockSpec((2, db, fc), lambda d, s, cut=i % UP_DEPTH_CUTS: (0, jnp.clip(d - cut * per_cut, 0, per_cut - 1), 0)) for i in range(len(outs))]
    else:
        outs = [jax.ShapeDtypeStruct((2, depth, width), BF16)]
        specs = [pl.BlockSpec((2, db, width), lambda d, s: (0, d, 0))]
    return pl.pallas_call(
        relayout_kernel,
        grid_spec=pltpu.PrefetchScalarGridSpec(
            num_scalar_prefetch=1, grid=(steps,),
            in_specs=[pl.BlockSpec((db, 2, width), lambda d, s: (d, 0, s[0]))],
            out_specs=specs),
        out_shape=outs,
        compiler_params=pltpu.CompilerParams(vmem_limit_bytes=40 * 2 ** 20),
        cost_estimate=pl.CostEstimate(flops=2_000_000_000, bytes_accessed=8 * depth * width, transcendentals=0),
    )(block, w_up)


def up_kernel(side_ref, za_ref, zo_ref, wa_ref, *rest):
    recv, (b_ref, g_ref) = rest[:-2], rest[-2:]
    cut = recv[0].shape[1]

    def part(t):
        acc = jnp.dot(za_ref[...], wa_ref[t], preferred_element_type=F32)
        for i, w_ref in enumerate(recv):
            acc = acc + jnp.dot(zo_ref[:, i * cut:(i + 1) * cut], w_ref[t], preferred_element_type=F32)
        return acc + b_ref[t:t + 1, :].astype(F32)

    g_ref[...] = (jax.nn.gelu(part(0), approximate=True) * part(1)).astype(BF16)


def up_gated(side, z_own, z_oth, w_all, w_recv, bias, chunk):
    rows, depth = z_own.shape
    width = w_recv[0].shape[2]
    row_block = rows // 2
    z_spec = pl.BlockSpec((row_block, depth), lambda r, s: (r, 0))
    return pl.pallas_call(
        up_kernel,
        grid_spec=pltpu.PrefetchScalarGridSpec(
            num_scalar_prefetch=1, grid=(2,),
            in_specs=[z_spec, z_spec, pl.BlockSpec((2, depth, width), lambda r, s: (0, 0, chunk))] + [pl.BlockSpec(w.shape, lambda r, s: (0, 0, 0)) for w in w_recv] + [pl.BlockSpec((2, width), lambda r, s: (0, chunk))],
            out_specs=pl.BlockSpec((row_block, width), lambda r, s: (r, 0))),
        out_shape=jax.ShapeDtypeStruct((rows, width), BF16),
        compiler_params=pltpu.CompilerParams(vmem_limit_bytes=40 * 2 ** 20),
        cost_estimate=pl.CostEstimate(flops=8 * rows * depth * width, bytes_accessed=8 * depth * width + 4 * rows * depth + 2 * rows * width, transcendentals=rows * width),
        name="upgate",
    )(side, z_own, z_oth, w_all, *w_recv, bias)


def qkv_kernel(block_ref, w_ref, h_ref, b_ref, *outs):
    prod = lax.dot_general(w_ref[...], h_ref[...], (((0,), (1,)), ((), ())), preferred_element_type=F32)
    if outs[0].dtype == F32:
        prod = prod + b_ref[...]
    each = outs[0].shape[0]
    for i, out in enumerate(outs):
        out[...] = prod[i * each:(i + 1) * each].astype(out.dtype)


def qkv_heads(block, w_qkv, hidden, bias, pieces, dtype):
    rows, depth = hidden.shape
    cols = w_qkv.shape[1] // 2
    row_block = rows // 4
    out = jax.ShapeDtypeStruct((cols // pieces, rows), dtype)
    return pl.pallas_call(
        qkv_kernel,
        grid_spec=pltpu.PrefetchScalarGridSpec(
            num_scalar_prefetch=1, grid=(rows // row_block,),
            in_specs=[pl.BlockSpec((depth, cols), lambda r, s: (0, s[0])), pl.BlockSpec((row_block, depth), lambda r, s: (r, 0)), pl.BlockSpec((cols, 1), lambda r, s: (s[0], 0))],
            out_specs=[pl.BlockSpec((cols // pieces, row_block), lambda r, s: (0, r))] * pieces),
        out_shape=[out] * pieces,
        compiler_params=pltpu.CompilerParams(vmem_limit_bytes=60 * 2 ** 20),
        cost_estimate=pl.CostEstimate(flops=2 * rows * depth * cols, bytes_accessed=2 * depth * (rows + cols) + 4 * rows * cols, transcendentals=0),
    )(block, w_qkv, hidden, bias)


def solution(mesh):
    cache_spec = P('dp', None, 'y', None)
    width_spec = P('x')
    in_specs = (P('dp', 'x'), P('x', 'y'), P('y'), P('y', 'x'), width_spec, width_spec, width_spec, P('x', None, 'y'), P(None, 'y'), P('y', 'x'), width_spec, width_spec, width_spec, cache_spec, cache_spec, P('dp'), P('dp'))
    out_specs = (P('dp', 'x'), cache_spec, cache_spec)
    swap_x = [(0, 1), (1, 0)]
    swap_core = [(i, i ^ 1) for i in range(4)]
    swap_chip = [(i, i ^ 2) for i in range(4)]

    def over_x(v):
        return lax.ppermute(v, 'x', swap_x)

    def over_core(v):
        return lax.ppermute(v, 'y', swap_core)

    def over_chip(v):
        return lax.ppermute(v, 'y', swap_chip)

    def layer(hidden, w_qkv, b_qkv, w_out, b_out, attn_gain, attn_shift, w_up, b_up, w_down, b_down, mlp_gain, mlp_shift, k_cache, v_cache, positions, lengths):
        rows, width = hidden.shape
        width_all = 2 * width
        _, local_heads, head_dim = k_cache.shape[1:]
        half_heads = local_heads // 2
        heads_c = half_heads // HEAD_CHUNKS
        side = lax.axis_index('x')
        y_index = lax.axis_index('y')
        side_arr = side[None].astype(jnp.int32)
        own_first = [side * half_heads + j * heads_c for j in range(HEAD_CHUNKS)]
        oth_first = [(1 - side) * half_heads + j * heads_c for j in range(HEAD_CHUNKS)]
        bias_col = b_qkv.astype(F32)[:, None]
        qkv_send = qkv_heads((1 - side)[None].astype(jnp.int32), w_qkv, hidden, bias_col, HEAD_CHUNKS, BF16)
        qkv_recv = [over_x(v) for v in qkv_send]
        hidden_late, _ = lax.optimization_barrier((hidden, qkv_send[0]))
        qkv_own = qkv_heads(side_arr, w_qkv, hidden_late, bias_col, HEAD_CHUNKS, F32)

        len_row = lengths[None]
        inv_freq = ROPE_BASE ** (-2.0 * jnp.arange(head_dim // 2, dtype=F32) / head_dim)
        angles = inv_freq[:, None] * positions.astype(F32)[None, :]
        cos_t, sin_t = jnp.cos(angles), jnp.sin(angles)

        f_half = w_up.shape[2] // 2
        w_down_own = lax.dynamic_slice_in_dim(w_down, side * f_half, f_half, 0)
        w_down_oth = lax.dynamic_slice_in_dim(w_down, (1 - side) * f_half, f_half, 0)
        w_out_own = lax.dynamic_slice_in_dim(w_out, side * half_heads * head_dim, half_heads * head_dim, 0)
        w_out_oth = lax.dynamic_slice_in_dim(w_out, (1 - side) * half_heads * head_dim, half_heads * head_dim, 0)

        w_up_early, _ = lax.optimization_barrier((w_up, qkv_own[0]))
        w_up_send = relayout_up((1 - side)[None].astype(jnp.int32), w_up_early, True)
        w_up_recv = [[over_x(w_up_send[i * UP_DEPTH_CUTS + d]) for d in range(UP_DEPTH_CUTS)] for i in range(UP_CHUNKS)]

        k_t = jnp.transpose(k_cache, (1, 2, 3, 0))
        v_t = jnp.transpose(v_cache, (1, 2, 3, 0))
        k_full = v_full = None
        attn_own, attn_recv, k_new, v_new = [], [], [], []
        for j in range(HEAD_CHUNKS):
            k_full, v_full, attn_c, k_c, v_c = attend_chunk(own_first[j][None].astype(jnp.int32), heads_c, qkv_own[j], qkv_recv[j], cos_t, sin_t, len_row, k_t, v_t, k_full, v_full)
            attn_own.append(attn_c)
            attn_recv.append(over_x(attn_c))
            k_new.append(k_c)
            v_new.append(v_c)
        attn_own = jnp.concatenate(attn_own, axis=0)
        attn_recv = jnp.concatenate(attn_recv, axis=0)
        w_up_late, _ = lax.optimization_barrier((w_up, attn_own))
        w_up_t, = relayout_up(side_arr, w_up_late, False)
        b_up_own = lax.dynamic_slice_in_dim(b_up, side * f_half, f_half, 1)

        quarter = rows // 4
        piece = quarter // STREAMS
        hid_q = lax.dynamic_slice_in_dim(hidden, y_index * quarter, quarter, 0)
        near = (0, 2, 1, 3)

        def reduce_scatter_y(part):
            two = part[:2 * piece].astype(F32) + over_core(part[2 * piece:].astype(BF16)).astype(F32)
            return two[:piece] + over_chip(two[piece:].astype(BF16)).astype(F32)

        def gather_y(val):
            both = jnp.concatenate([val, over_chip(val)], axis=0)
            return jnp.concatenate([both, over_core(both)], axis=0)

        def norm(h_val, gain, shift):
            mean_l = jnp.mean(h_val, axis=1)
            dev = jnp.sum(jnp.square(h_val - mean_l[:, None]), axis=1)
            other = over_x(jnp.stack([mean_l, dev]))
            mean_row = 0.5 * (mean_l + other[0])
            var_row = (dev + other[1] + (width / 2) * jnp.square(mean_l - other[0])) / width_all
            scaled = (h_val - mean_row[:, None]) * lax.rsqrt(var_row + LN_EPS)[:, None]
            return (scaled * gain.astype(F32) + shift.astype(F32)).astype(BF16)

        k_recv = over_x(jnp.concatenate(k_new, axis=0))
        v_recv = over_x(jnp.concatenate(v_new, axis=0))
        outs = []
        for r in range(STREAMS):
            starts = [(y_index ^ i) * quarter + r * piece for i in near]

            def project(attn_t, w):
                rel = jnp.concatenate([lax.dynamic_slice_in_dim(attn_t, s, piece, 1) for s in starts], axis=1)
                return lax.dot_general(rel, w, (((0,), (0,)), ((), ())), preferred_element_type=F32)

            part = project(attn_own, w_out_own)
            proj_sum = reduce_scatter_y(part + project(attn_recv, w_out_oth))
            h_attn = DEEP_ALPHA * hid_q[r * piece:(r + 1) * piece].astype(F32) + proj_sum + b_out.astype(F32)
            z_q = norm(h_attn, attn_gain, attn_shift)
            z_own = gather_y(z_q)
            z_oth = gather_y(over_x(z_q))
            g_own, g_recv = [], []
            for i in range(UP_CHUNKS):
                g_own.append(up_gated(side_arr, z_own, z_oth, w_up_t, w_up_recv[i], b_up_own, i))
                g_recv.append(over_x(g_own[-1]))
            down = jnp.dot(jnp.concatenate(g_own, axis=1), w_down_own, preferred_element_type=F32)
            down = down + jnp.dot(jnp.concatenate(g_recv, axis=1), w_down_oth, preferred_element_type=F32)
            down_sum = reduce_scatter_y(down)
            h_mlp = DEEP_ALPHA * z_q.astype(F32) + down_sum + b_down.astype(F32)
            outs.append(gather_y(norm(h_mlp, mlp_gain, mlp_shift)).reshape(4, piece, width))
        result = jnp.stack(outs, axis=1)
        order = [jnp.where((y_index ^ j) == 1, 2, jnp.where((y_index ^ j) == 2, 1, y_index ^ j)) for j in range(4)]
        result = jnp.concatenate([lax.dynamic_index_in_dim(result, o, 0, keepdims=False).reshape(quarter, width) for o in order], axis=0)

        cut = half_heads * head_dim // 2
        for i in range(2):
            first = (oth_first[0] + i * half_heads // 2)[None].astype(jnp.int32)
            k_full = insert_other(first, len_row, k_recv[i * cut:(i + 1) * cut], k_t, k_full)
            v_full = insert_other(first, len_row, v_recv[i * cut:(i + 1) * cut], v_t, v_full)
        return result, jnp.transpose(k_full, (3, 0, 1, 2)), jnp.transpose(v_full, (3, 0, 1, 2))

    return jax.shard_map(layer, mesh=mesh, in_specs=in_specs, out_specs=out_specs, check_vma=False)
```
